32 devices in a mesh: emb: 4 (over x, core), heads: 8 (over z, y).
Axes of the slice: x: 2, y: 2, z: 4, core: 2. Of those that a mesh axis runs over, the one named last changes fastest.
Arguments:
- hidden_in: bfloat16 [16, 8192], P(None, 'emb'), may hold values from -6 to 6
- w_z: bfloat16 [8192, 16384], P('emb', 'heads'), may hold values from -0.0625 to 0.0625
- w_x: bfloat16 [8192, 16384], P('emb', 'heads'), may hold values from -0.0625 to 0.0625
- w_bc: bfloat16 [8192, 4096], P('emb'), may hold values from -0.0625 to 0.0625
- w_dt: bfloat16 [8192, 256], P('emb', 'heads'), may hold values from -0.0625 to 0.0625
- dt_bias: float32 [256], P('heads'), may hold values from -4 to -1
- a_log: float32 [256], P('heads'), may hold values from 0 to 2.77
- skip_gain: float32 [256], P('heads'), may hold values from 0.5 to 2
- conv_x: bfloat16 [16, 3, 16384], P('emb', None, 'heads'), may hold values from -6 to 6
- conv_bc: bfloat16 [16, 3, 4096], P('emb'), may hold values from -6 to 6
- conv_wx: float32 [4, 16384], P(None, 'heads'), may hold values from -3 to 3
- conv_wbc: float32 [4, 4096], replicated, may hold values from -3 to 3
- ssm_state: float32 [16, 256, 64, 256], P('emb', 'heads'), may hold values from -0.6 to 0.6
- norm_gain: float32 [16384], P('heads'), may hold values from 0.5 to 1.5
- w_out: bfloat16 [16384, 8192], P('heads', 'emb'), may hold values from -0.046875 to 0.046875
Outputs:
- mixed: bfloat16 [16, 8192], P(None, 'emb')
- new_state: float32 [16, 256, 64, 256], P('emb', 'heads')
The draws below stay inside these ranges and needn't reach their ends.
All inputs are finite; a program needn't handle non-finite values.
Results may differ from the reference program's by a relative error of at most 0.0051.
Values may be sent and summed in bfloat16 or wider, within the bound.
A program may use at most 128 MiB of HBM per device.

```python
import jax
import jax.numpy as jnp
from jax import lax

D = 8192
H = 256
P_SIZE = 64
N = 256
G = 8
KERNEL = 4
BATCH = 16
DI = 16384


def level_of(own_key, extent, shards, low, largest):
    def one(axis_at, shards_of):
        draws = jax.random.uniform(jax.random.fold_in(jax.random.fold_in(own_key, 6), axis_at), (shards_of,), jnp.float32, low / len(shards), largest / len(shards))
        return jnp.repeat(jnp.exp(draws), extent[axis_at] // shards_of).reshape((-1,) + (1,) * (len(extent) - axis_at - 1))

    gain = one(*shards[0])
    for cut in shards[1:]:
        gain = gain * one(*cut)
    return gain


def normal_values(key, shape, spread, reach, cuts=(), held_as=jnp.bfloat16):
    entries = jax.random.normal(key, shape, jnp.float32) * spread
    if len(cuts) > 0:
        entries = level_of(key, shape, cuts, -0.22, 0.18) * entries
    return jnp.clip(entries, min=-reach, max=reach).astype(held_as)


def setup_inputs(seed: int = 0) -> dict:
    splits = jax.random.split(jax.random.key(seed), 16)
    hidden_in = normal_values(splits[0], (BATCH, D), 1.0, 6.0, ((1, 4),))
    w_z = normal_values(splits[1], (D, DI), D ** -0.5, 0.0625, ((0, 4), (1, 8)))
    w_x = normal_values(splits[2], (D, DI), D ** -0.5, 0.0625, ((0, 4), (1, 8)))
    w_bc = normal_values(splits[3], (D, 2 * G * N), D ** -0.5, 0.0625, ((0, 4),))
    w_dt = normal_values(splits[4], (D, H), D ** -0.5, 0.0625, ((0, 4), (1, 8)))
    dt_bias = jnp.clip(-4.0 + 3.0 * jax.random.uniform(splits[5], (H,), jnp.float32) ** level_of(splits[5], (H,), ((0, 8),), -0.2, 0.2), -4.0, -1.0)
    a_log = jnp.clip(2.77 * jax.random.uniform(splits[6], (H,), jnp.float32) ** level_of(splits[6], (H,), ((0, 8),), -0.2, 0.2), 0.0, 2.77)
    skip_gain = jnp.clip(0.5 + 1.5 * jax.random.uniform(splits[7], (H,), jnp.float32) ** level_of(splits[7], (H,), ((0, 8),), -0.2, 0.2), 0.5, 2.0)
    conv_x = normal_values(splits[8], (BATCH, KERNEL - 1, DI), 1.0, 6.0, ((0, 4), (2, 8)))
    conv_bc = normal_values(splits[9], (BATCH, KERNEL - 1, 2 * G * N), 1.0, 6.0, ((0, 4),))
    conv_wx = normal_values(splits[10], (KERNEL, DI), 0.5, 3.0, ((1, 8),), jnp.float32)
    conv_wbc = normal_values(splits[11], (KERNEL, 2 * G * N), 0.5, 3.0, (), jnp.float32)
    ssm_state = normal_values(splits[12], (BATCH, H, P_SIZE, N), 0.1, 0.6, ((0, 4), (1, 8)), jnp.float32)
    norm_gain = jnp.clip(1.0 + 0.1 * jax.random.normal(splits[13], (DI,), jnp.float32), 0.5, 1.5)
    w_out = normal_values(splits[14], (DI, D), DI ** -0.5, 0.046875, ((0, 8), (1, 4)))
    return dict(hidden_in=hidden_in, w_z=w_z, w_x=w_x, w_bc=w_bc, w_dt=w_dt, dt_bias=dt_bias, a_log=a_log, skip_gain=skip_gain, conv_x=conv_x, conv_bc=conv_bc, conv_wx=conv_wx, conv_wbc=conv_wbc, ssm_state=ssm_state, norm_gain=norm_gain, w_out=w_out)


def reference(hidden_in, w_z, w_x, w_bc, w_dt, dt_bias, a_log, skip_gain, conv_x, conv_bc, conv_wx, conv_wbc, ssm_state, norm_gain, w_out):
    z_pre = jnp.dot(hidden_in, w_z, preferred_element_type=jnp.float32)
    x_pre = jnp.dot(hidden_in, w_x, preferred_element_type=jnp.float32)
    bc_pre = jnp.dot(hidden_in, w_bc, preferred_element_type=jnp.float32)
    dt_pre = jnp.dot(hidden_in, w_dt, preferred_element_type=jnp.float32)
    window_x = jnp.concatenate([conv_x.astype(jnp.float32), x_pre[:, None, :]], axis=1)
    x_conv = jax.nn.silu(lax.optimization_barrier(jnp.sum(window_x * conv_wx[None], axis=1)))
    window_bc = jnp.concatenate([conv_bc.astype(jnp.float32), bc_pre[:, None, :]], axis=1)
    bc_conv = jax.nn.silu(lax.optimization_barrier(jnp.sum(window_bc * conv_wbc[None], axis=1)))
    batch_all = hidden_in.shape[0]
    bc_view = bc_conv.reshape(batch_all, 2, G, N)
    b_heads = jnp.repeat(bc_view[:, 0], H // G, axis=1)
    c_heads = jnp.repeat(bc_view[:, 1], H // G, axis=1)
    step_size = jax.nn.softplus(dt_pre + dt_bias[None])
    decay_rate = jnp.exp(-jnp.exp(a_log)[None] * step_size)
    x_heads = x_conv.reshape(batch_all, H, P_SIZE)
    new_state = decay_rate[:, :, None, None] * ssm_state + (step_size[:, :, None] * x_heads)[..., None] * b_heads[:, :, None, :]
    readout = jnp.einsum('bhpn,bhn->bhp', new_state, c_heads, precision=lax.Precision.HIGHEST)
    readout = readout + skip_gain[None, :, None] * x_heads
    gated = readout.reshape(batch_all, H * P_SIZE) * jax.nn.silu(z_pre)
    grouped = gated.reshape(batch_all, G, H * P_SIZE // G)
    mean_sq = lax.optimization_barrier(jnp.mean(grouped * grouped, axis=-1))
    inv_rms = lax.rsqrt(mean_sq + 1e-05)
    normed = ((grouped * inv_rms[..., None]).reshape(batch_all, H * P_SIZE) * norm_gain[None]).astype(jnp.bfloat16)
    mixed = jnp.dot(normed, w_out, preferred_element_type=jnp.float32).astype(jnp.bfloat16)
    return (mixed, new_state)
```

```python
import functools

import jax
import jax.numpy as jnp
from jax import lax
from jax.experimental import pallas as pl
from jax.experimental.pallas import tpu as pltpu
from jax.sharding import PartitionSpec as P

H = 256
P_SIZE = 64
N = 256
G = 8
LANES = 128
DEPTH = 6
MESH = pl.DeviceIdType.MESH
F32 = jnp.float32
BF16 = jnp.bfloat16


def silu(v):
    return v / (1.0 + jnp.exp(-v))


def softplus(v):
    return jnp.maximum(v, 0.0) + jnp.log1p(jnp.exp(-jnp.abs(v)))


def split3(v):
    high = v.astype(BF16)
    rest = v - high.astype(F32)
    mid = rest.astype(BF16)
    low = (rest - mid.astype(F32)).astype(BF16)
    return high, mid, low


def kernel(
    dims,
    hidden_ref,
    dtb_ref,
    alog_ref,
    skip_ref,
    convx_ref,
    convwx_ref,
    gain_ref,
    wz_hbm,
    wx_hbm,
    wbc_hbm,
    wdt_hbm,
    convbc_hbm,
    convwbc_hbm,
    state_hbm,
    wout_hbm,
    out_ref,
    st_ref,
    wz_v,
    wx_v,
    wbc_v,
    wdt_v,
    convbc_v,
    convwbc_v,
    wout_v,
    xsend,
    xrecv,
    zsend,
    zrecv,
    cols_v,
    read_v,
    xc_v,
    ag_v,
    rs_send,
    rs_recv,
    fin_send,
    fin_v,
    sq_send,
    sq_recv,
    dma_sem,
    x_ss,
    x_rs,
    z_ss,
    z_rs,
    a_ss,
    a_rs,
    r_ss,
    r_rs,
    f_ss,
    f_rs,
    q_ss,
    q_rs,
):
    n_emb, n_heads, batch, bd, di, hd, cols, chunk, ochunk, fused, span = dims
    e = lax.axis_index("emb")
    h = lax.axis_index("heads")
    group = h // span

    def emb_peer(o):
        return lax.rem(e + o, n_emb)

    def head_peer(o):
        return lax.rem(h + o, n_heads)

    copies = {}
    order = []

    def stream(name, src, dst):
        copies[name] = pltpu.make_async_copy(src, dst, dma_sem.at[len(order)])
        order.append(name)

    for half in range(2):
        off = pl.multiple_of(half * G * N + group * N, N)
        stream(("bc", half), wbc_hbm.at[:, pl.ds(off, N)], wbc_v.at[half])
    stream(("dt", 0), wdt_hbm, wdt_v)
    for half in range(2):
        off = pl.multiple_of(half * G * N + group * N, N)
        stream(("cb", half), convbc_hbm.at[:, :, pl.ds(off, N)], convbc_v.at[half])
        stream(("cw", half), convwbc_hbm.at[:, pl.ds(off, N)], convwbc_v.at[half])
    n_chunk = di // chunk
    for c in range(n_chunk):
        stream(("x", c), wx_hbm.at[:, pl.ds(c * chunk, chunk)], wx_v.at[c])
    for c in range(n_chunk):
        stream(("z", c), wz_hbm.at[:, pl.ds(c * chunk, chunk)], wz_v.at[c])
    for b in range(bd):
        stream(("s", b), state_hbm.at[b], st_ref.at[b])
    n_out = cols // ochunk
    for i in range(n_out):
        at = lax.rem(h + i + 1, n_heads) if fused else i
        off = pl.multiple_of(at * ochunk, ochunk)
        stream(("o", i), wout_hbm.at[:, pl.ds(off, ochunk)], wout_v.at[i])
    started = [0]

    def advance():
        if started[0] < len(order):
            copies[order[started[0]]].start()
            started[0] += 1

    def ready(name):
        copies[name].wait()
        advance()

    for _ in range(DEPTH + 6):
        advance()

    barrier = pltpu.get_barrier_semaphore()
    for o in range(1, n_emb):
        pl.semaphore_signal(barrier, inc=1, device_id={"emb": emb_peer(o)}, device_id_type=MESH)
    n_greet = n_emb - 1
    if fused:
        for o in range(1, n_heads):
            pl.semaphore_signal(
                barrier, inc=1, device_id={"heads": head_peer(o)}, device_id_type=MESH
            )
        n_greet += n_heads - 1
    elif span > 1:
        for o in range(1, span):
            pl.semaphore_signal(
                barrier,
                inc=1,
                device_id={"heads": group * span + lax.rem(h % span + o, span)},
                device_id_type=MESH,
            )
        n_greet += span - 1

    hidden = hidden_ref[...]

    def project(weights, send, at, width):
        part = jnp.dot(hidden, weights, preferred_element_type=F32)
        for peer in range(n_emb):
            send[peer, :, at : at + width] = part[peer * bd : (peer + 1) * bd]

    heads_at = lax.broadcasted_iota(jnp.int32, (hd, di), 0)
    chans_at = lax.broadcasted_iota(jnp.int32, (hd, di), 1)
    lower = heads_at * P_SIZE
    expand = jnp.where((chans_at >= lower) & (chans_at < lower + P_SIZE), 1.0, 0.0).astype(BF16)

    def conv_prev(values, taps, k):
        rows = [
            jnp.sum(values[b].astype(F32) * taps[0:k], axis=0, keepdims=True) for b in range(bd)
        ]
        return jnp.concatenate(rows, axis=0)

    k_prev = convx_ref.shape[1]
    x_base = conv_prev(convx_ref, convwx_ref[...], k_prev)

    for half in range(2):
        ready(("bc", half))
        project(wbc_v[half], xsend, di + half * N, N)
    ready(("dt", 0))
    xsend[:, :, di + 2 * N :] = jnp.zeros((n_emb, bd, LANES), F32)
    project(wdt_v[...], xsend, di + 2 * N, hd)
    bc_base = []
    for half in range(2):
        ready(("cb", half))
        ready(("cw", half))
        bc_base.append(conv_prev(convbc_v.at[half], convwbc_v[half], k_prev))
    for c in range(n_chunk):
        ready(("x", c))
        project(wx_v[c], xsend, c * chunk, chunk)

    pl.semaphore_wait(barrier, n_greet)

    def send_emb(src, dst, ss, rs):
        made = []
        for o in range(n_emb - 1, 0, -1):
            peer = emb_peer(o)
            copy = pltpu.make_async_remote_copy(
                src_ref=src.at[peer],
                dst_ref=dst.at[o - 1],
                send_sem=ss.at[o - 1],
                recv_sem=rs.at[o - 1],
                device_id={"emb": peer},
                device_id_type=MESH,
            )
            copy.start()
            made.append(copy)
        return made

    x_copies = send_emb(xsend, xrecv, x_ss, x_rs)
    for c in range(n_chunk):
        ready(("z", c))
        project(wz_v[c], zsend, c * chunk, chunk)
    z_copies = send_emb(zsend, zrecv, z_ss, z_rs)

    for copy in x_copies:
        copy.wait_recv()
    xall = xsend[e]
    for o in range(n_emb - 1):
        xall = xall + xrecv[o]
    x_conv = silu(x_base + xall[:, 0:di] * convwx_ref[k_prev : k_prev + 1, :])
    bc = []
    for half in range(2):
        pre = xall[:, di + half * N : di + (half + 1) * N]
        bc.append(silu(bc_base[half] + pre * convwbc_v[half, k_prev : k_prev + 1, :]))
    b_group, c_group = bc
    dt_pre = xall[:, di + 2 * N : di + 2 * N + hd]
    step = softplus(dt_pre + dtb_ref[...])
    decay = jnp.exp(-jnp.exp(alog_ref[...]) * step)
    skip = jnp.broadcast_to(skip_ref[...], (bd, hd))
    by_head = jnp.concatenate([step, decay, skip], axis=0)
    by_chan = sum(jnp.dot(part, expand, preferred_element_type=F32) for part in split3(by_head))
    step_c = by_chan[0:bd]
    decay_c = by_chan[bd : 2 * bd]
    skip_c = by_chan[2 * bd : 3 * bd]
    rows = jnp.concatenate([step_c * x_conv, decay_c], axis=0)
    cols_v[...] = jnp.transpose(rows)
    xc_v[...] = skip_c * x_conv
    c_high, c_low, _ = split3(c_group)
    c_both = jnp.concatenate([c_high.astype(F32), c_low.astype(F32)], axis=0).astype(BF16)

    rows_at = 256 if di % 256 == 0 else di
    for b in range(bd):
        ready(("s", b))
        b_row = b_group[b : b + 1, :]

        def update(i, carry, b=b, b_row=b_row):
            at = pl.ds(pl.multiple_of(i * rows_at, rows_at), rows_at)
            xcol = cols_v[at, b : b + 1]
            dcol = cols_v[at, bd + b : bd + b + 1]
            new = dcol * st_ref[b, at, :] + xcol * b_row
            st_ref[b, at, :] = new
            got = lax.dot_general(
                c_both, new.astype(BF16), (((1,), (1,)), ((), ())), preferred_element_type=F32
            )
            read_v[b : b + 1, at] = got[b : b + 1, :] + got[bd + b : bd + b + 1, :]
            return carry

        lax.fori_loop(0, di // rows_at, update, 0)

    for copy in z_copies:
        copy.wait_recv()
    zall = zsend[e]
    for o in range(n_emb - 1):
        zall = zall + zrecv[o]
    gated = (read_v[...] + xc_v[...]) * silu(zall)
    total = jnp.sum(gated * gated, axis=1, keepdims=True)
    q_copies = []
    if span > 1:
        sq_send[...] = jnp.broadcast_to(total, (bd, LANES))
        for o in range(1, span):
            copy = pltpu.make_async_remote_copy(
                src_ref=sq_send,
                dst_ref=sq_recv.at[o - 1],
                send_sem=q_ss.at[o - 1],
                recv_sem=q_rs.at[o - 1],
                device_id={"heads": group * span + lax.rem(h % span + o, span)},
                device_id_type=MESH,
            )
            copy.start()
            q_copies.append(copy)
        for o, copy in enumerate(q_copies):
            copy.wait_recv()
            total = total + sq_recv[o][:, 0:1]
    inv_rms = lax.rsqrt(total / (H * P_SIZE // G) + 1e-05)
    normed = (gated * inv_rms * gain_ref[...]).astype(BF16)
    ag_v[e] = normed
    a_copies = []
    for o in range(n_emb - 1, 0, -1):
        copy = pltpu.make_async_remote_copy(
            src_ref=ag_v.at[e],
            dst_ref=ag_v.at[e],
            send_sem=a_ss.at[o - 1],
            recv_sem=a_rs.at[o - 1],
            device_id={"emb": emb_peer(o)},
            device_id_type=MESH,
        )
        copy.start()
        a_copies.append(copy)
    for copy in a_copies:
        copy.wait_recv()
    whole = jnp.concatenate([ag_v[i].astype(F32) for i in range(n_emb)], axis=0).astype(BF16)

    last = []
    own = None
    for i in range(n_out):
        ready(("o", i))
        part = jnp.dot(whole, wout_v[i], preferred_element_type=F32)
        if not fused:
            out_ref[:, i * ochunk : (i + 1) * ochunk] = part
        elif i < n_out - 1:
            rs_send[i] = part.astype(BF16)
            copy = pltpu.make_async_remote_copy(
                src_ref=rs_send.at[i],
                dst_ref=rs_recv.at[i],
                send_sem=r_ss.at[i],
                recv_sem=r_rs.at[i],
                device_id={"heads": head_peer(i + 1)},
                device_id_type=MESH,
            )
            copy.start()
            last.append(copy)
        else:
            own = part
    f_copies = []
    if fused:
        for i, copy in enumerate(last):
            copy.wait_recv()
            own = own + rs_recv[i].astype(F32)
        fin_send[...] = own.astype(BF16)
        for o in range(1, n_heads):
            copy = pltpu.make_async_remote_copy(
                src_ref=fin_send,
                dst_ref=fin_v.at[h],
                send_sem=f_ss.at[o - 1],
                recv_sem=f_rs.at[o - 1],
                device_id={"heads": head_peer(o)},
                device_id_type=MESH,
            )
            copy.start()
            f_copies.append(copy)
        fin_v[h] = fin_send[...]
        for copy in f_copies:
            copy.wait_recv()
        for i in range(n_heads):
            out_ref[:, i * ochunk : (i + 1) * ochunk] = fin_v[i]
    for copy in x_copies + z_copies + q_copies + a_copies + last + f_copies:
        copy.wait_send()


def on_device(
    hidden_in,
    w_z,
    w_x,
    w_bc,
    w_dt,
    dt_bias,
    a_log,
    skip_gain,
    conv_x,
    conv_bc,
    conv_wx,
    conv_wbc,
    ssm_state,
    norm_gain,
    w_out,
):
    n_emb = lax.axis_size("emb")
    n_heads = lax.axis_size("heads")
    span = n_heads // G
    batch, depth = hidden_in.shape
    bd = conv_x.shape[0]
    k_prev = conv_x.shape[1]
    di = w_x.shape[1]
    hd = w_dt.shape[1]
    cols = w_out.shape[1]
    fused = cols % (n_heads * LANES) == 0
    chunk = min(512, di)
    ochunk = cols // n_heads if fused else min(256, cols)
    dims = (n_emb, n_heads, batch, bd, di, hd, cols, chunk, ochunk, fused, span)
    n_chunk = di // chunk
    n_out = cols // ochunk
    x_cols = di + 2 * N + LANES
    n_streams = 7 + 2 * n_chunk + bd + n_out
    vm = pl.BlockSpec(memory_space=pltpu.VMEM)
    hbm = pl.BlockSpec(memory_space=pl.ANY)
    dma = pltpu.SemaphoreType.DMA
    rs_n = max(n_heads - 1, 1) if fused else 1
    rs_shape = (batch, ochunk) if fused else (batch, LANES)
    fin_n = n_heads if fused else 1
    e_n = max(n_emb - 1, 1)
    q_n = max(span - 1, 1)
    out, new_state = pl.pallas_call(
        functools.partial(kernel, dims),
        out_shape=(
            jax.ShapeDtypeStruct((batch, cols), BF16 if fused else F32),
            pltpu.VMEM((bd, di, N), F32),
        ),
        in_specs=[vm] * 7 + [hbm] * 8,
        out_specs=(vm, vm),
        scratch_shapes=[
            pltpu.VMEM((n_chunk, depth, chunk), BF16),
            pltpu.VMEM((n_chunk, depth, chunk), BF16),
            pltpu.VMEM((2, depth, N), BF16),
            pltpu.VMEM((depth, hd), BF16),
            pltpu.VMEM((2, bd, k_prev, N), BF16),
            pltpu.VMEM((2, k_prev + 1, N), F32),
            pltpu.VMEM((n_out, w_out.shape[0], ochunk), BF16),
            pltpu.VMEM((n_emb, bd, x_cols), F32),
            pltpu.VMEM((e_n, bd, x_cols), F32),
            pltpu.VMEM((n_emb, bd, di), F32),
            pltpu.VMEM((e_n, bd, di), F32),
            pltpu.VMEM((di, 2 * bd), F32),
            pltpu.VMEM((bd, di), F32),
            pltpu.VMEM((bd, di), F32),
            pltpu.VMEM((n_emb, bd, di), BF16),
            pltpu.VMEM((rs_n,) + rs_shape, BF16),
            pltpu.VMEM((rs_n,) + rs_shape, BF16),
            pltpu.VMEM(rs_shape, BF16),
            pltpu.VMEM((fin_n,) + rs_shape, BF16),
            pltpu.VMEM((bd, LANES), F32),
            pltpu.VMEM((q_n, bd, LANES), F32),
            dma((n_streams,)),
            dma((e_n,)),
            dma((e_n,)),
            dma((e_n,)),
            dma((e_n,)),
            dma((e_n,)),
            dma((e_n,)),
            dma((rs_n,)),
            dma((rs_n,)),
            dma((rs_n,)),
            dma((rs_n,)),
            dma((q_n,)),
            dma((q_n,)),
        ],
        compiler_params=pltpu.CompilerParams(
            collective_id=0, has_side_effects=True, vmem_limit_bytes=44 * 1024 * 1024
        ),
    )(
        hidden_in,
        dt_bias.reshape(1, hd),
        a_log.reshape(1, hd),
        skip_gain.reshape(1, hd),
        conv_x,
        conv_wx,
        norm_gain.reshape(1, di),
        w_z,
        w_x,
        w_bc,
        w_dt,
        conv_bc,
        conv_wbc,
        ssm_state.reshape(bd, di, N),
        w_out,
    )
    mixed = out if fused else lax.psum(out, "heads").astype(BF16)
    return (mixed, new_state.reshape(bd, hd, P_SIZE, N))


def solution(mesh):
    in_specs = (
        P(None, "emb"),
        P("emb", "heads"),
        P("emb", "heads"),
        P("emb", None),
        P("emb", "heads"),
        P("heads"),
        P("heads"),
        P("heads"),
        P("emb", None, "heads"),
        P("emb", None, None),
        P(None, "heads"),
        P(),
        P("emb", "heads", None, None),
        P("heads"),
        P("heads", "emb"),
    )
    out_specs = (P(None, "emb"), P("emb", "heads", None, None))
    return jax.shard_map(
        on_device, mesh=mesh, in_specs=in_specs, out_specs=out_specs, check_vma=False
    )
```

```python
import functools

import jax
import jax.numpy as jnp
from jax import lax
from jax.experimental import pallas as pl
from jax.experimental.pallas import tpu as pltpu
from jax.sharding import PartitionSpec as P

H = 256
P_SIZE = 64
N = 256
G = 8
LANES = 128
DEPTH = 6
MESH = pl.DeviceIdType.MESH
F32 = jnp.float32
BF16 = jnp.bfloat16


def silu(v):
    return v / (1.0 + jnp.exp(-v))


def softplus(v):
    return jnp.maximum(v, 0.0) + jnp.log1p(jnp.exp(-jnp.abs(v)))


def split3(v):
    high = v.astype(BF16)
    rest = v - high.astype(F32)
    mid = rest.astype(BF16)
    low = (rest - mid.astype(F32)).astype(BF16)
    return high, mid, low


def kernel(
    dims,
    hidden_hbm,
    dtb_hbm,
    alog_hbm,
    skip_hbm,
    convx_hbm,
    convwx_hbm,
    gain_hbm,
    wz_hbm,
    wx_hbm,
    wbc_hbm,
    wdt_hbm,
    convbc_hbm,
    convwbc_hbm,
    state_hbm,
    wout_hbm,
    out_ref,
    st_ref,
    hidden_ref,
    dtb_ref,
    alog_ref,
    skip_ref,
    convx_v,
    convwx_ref,
    gain_ref,
    wz_v,
    wx_v,
    wbc_v,
    wdt_v,
    convbc_v,
    convwbc_v,
    wout_v,
    xsend,
    xrecv,
    zsend,
    zrecv,
    cols_v,
    read_v,
    xc_v,
    ag_v,
    rs_send,
    rs_recv,
    fin_send,
    fin_v,
    sq_send,
    sq_recv,
    dma_sem,
    x_ss,
    x_rs,
    z_ss,
    z_rs,
    a_ss,
    a_rs,
    r_ss,
    r_rs,
    f_ss,
    f_rs,
    q_ss,
    q_rs,
):
    n_emb, n_heads, batch, bd, di, hd, cols, chunk, ochunk, fused, span = dims
    e = lax.axis_index("emb")
    h = lax.axis_index("heads")
    group = h // span

    def emb_peer(o):
        return lax.rem(e + o, n_emb)

    def head_peer(o):
        return lax.rem(h + o, n_heads)

    copies = {}
    order = []

    def stream(name, src, dst):
        copies[name] = pltpu.make_async_copy(src, dst, dma_sem.at[len(order)])
        order.append(name)

    stream("hidden", hidden_hbm, hidden_ref)
    for half in range(2):
        off = pl.multiple_of(half * G * N + group * N, N)
        stream(("bc", half), wbc_hbm.at[:, pl.ds(off, N)], wbc_v.at[half])
    stream(("dt", 0), wdt_hbm, wdt_v)
    for half in range(2):
        off = pl.multiple_of(half * G * N + group * N, N)
        stream(("cb", half), convbc_hbm.at[:, :, pl.ds(off, N)], convbc_v.at[half])
        stream(("cw", half), convwbc_hbm.at[:, pl.ds(off, N)], convwbc_v.at[half])
    stream("dtb", dtb_hbm, dtb_ref)
    stream("alog", alog_hbm, alog_ref)
    stream("skip", skip_hbm, skip_ref)
    stream("convx", convx_hbm, convx_v)
    stream("convwx", convwx_hbm, convwx_ref)
    stream("gain", gain_hbm, gain_ref)
    n_chunk = di // chunk
    for c in range(n_chunk):
        stream(("x", c), wx_hbm.at[:, pl.ds(c * chunk, chunk)], wx_v.at[c])
    for c in range(n_chunk):
        stream(("z", c), wz_hbm.at[:, pl.ds(c * chunk, chunk)], wz_v.at[c])
    for b in range(bd):
        stream(("s", b), state_hbm.at[b], st_ref.at[b])
    n_out = cols // ochunk
    for i in range(n_out):
        at = lax.rem(h + i + 1, n_heads) if fused else i
        off = pl.multiple_of(at * ochunk, ochunk)
        stream(("o", i), wout_hbm.at[:, pl.ds(off, ochunk)], wout_v.at[i])
    started = [0]

    def advance():
        if started[0] < len(order):
            copies[order[started[0]]].start()
            started[0] += 1

    def ready(name):
        copies[name].wait()
        advance()

    for _ in range(DEPTH + 12):
        advance()

    barrier = pltpu.get_barrier_semaphore()
    for o in range(1, n_emb):
        pl.semaphore_signal(barrier, inc=1, device_id={"emb": emb_peer(o)}, device_id_type=MESH)
    n_greet = n_emb - 1
    if fused:
        for o in range(1, n_heads):
            pl.semaphore_signal(
                barrier, inc=1, device_id={"heads": head_peer(o)}, device_id_type=MESH
            )
        n_greet += n_heads - 1
    elif span > 1:
        for o in range(1, span):
            pl.semaphore_signal(
                barrier,
                inc=1,
                device_id={"heads": group * span + lax.rem(h % span + o, span)},
                device_id_type=MESH,
            )
        n_greet += span - 1

    ready("hidden")
    hidden = hidden_ref[...]

    def project(weights, send, at, width):
        part = jnp.dot(hidden, weights, preferred_element_type=F32)
        for peer in range(n_emb):
            send[peer, :, at : at + width] = part[peer * bd : (peer + 1) * bd]

    heads_at = lax.broadcasted_iota(jnp.int32, (hd, di), 0)
    chans_at = lax.broadcasted_iota(jnp.int32, (hd, di), 1)
    lower = heads_at * P_SIZE
    expand = jnp.where((chans_at >= lower) & (chans_at < lower + P_SIZE), 1.0, 0.0).astype(BF16)

    k_prev = convx_v.shape[0]

    def conv_prev(values, taps):
        return sum(values[k].astype(F32) * taps[k : k + 1, :] for k in range(k_prev))

    for half in range(2):
        ready(("bc", half))
        project(wbc_v[half], xsend, di + half * N, N)
    ready(("dt", 0))
    xsend[:, :, di + 2 * N :] = jnp.zeros((n_emb, bd, LANES), F32)
    part = lax.dot_general(
        hidden, wdt_v[...], (((1,), (1,)), ((), ())), preferred_element_type=F32
    )
    for peer in range(n_emb):
        xsend[peer, :, di + 2 * N : di + 2 * N + hd] = part[peer * bd : (peer + 1) * bd]
    bc_base = []
    for half in range(2):
        ready(("cb", half))
        ready(("cw", half))
        bc_base.append(conv_prev(convbc_v.at[half], convwbc_v[half]))
    for name in ("dtb", "alog", "skip", "convx", "convwx", "gain"):
        ready(name)
    x_base = conv_prev(convx_v, convwx_ref[...])
    for c in range(n_chunk):
        ready(("x", c))
        project(wx_v[c], xsend, c * chunk, chunk)

    pl.semaphore_wait(barrier, n_greet)

    def send_emb(src, dst, ss, rs):
        made = []
        for o in range(n_emb - 1, 0, -1):
            peer = emb_peer(o)
            copy = pltpu.make_async_remote_copy(
                src_ref=src.at[peer],
                dst_ref=dst.at[o - 1],
                send_sem=ss.at[o - 1],
                recv_sem=rs.at[o - 1],
                device_id={"emb": peer},
                device_id_type=MESH,
            )
            copy.start()
            made.append(copy)
        return made

    x_copies = send_emb(xsend, xrecv, x_ss, x_rs)
    for c in range(n_chunk):
        ready(("z", c))
        project(wz_v[c], zsend, c * chunk, chunk)
    z_copies = send_emb(zsend, zrecv, z_ss, z_rs)

    for copy in x_copies:
        copy.wait_recv()
    xall = xsend[e]
    for o in range(n_emb - 1):
        xall = xall + xrecv[o]
    x_conv = silu(x_base + xall[:, 0:di] * convwx_ref[k_prev : k_prev + 1, :])
    bc = []
    for half in range(2):
        pre = xall[:, di + half * N : di + (half + 1) * N]
        bc.append(silu(bc_base[half] + pre * convwbc_v[half, k_prev : k_prev + 1, :]))
    b_group, c_group = bc
    dt_pre = xall[:, di + 2 * N : di + 2 * N + hd]
    step = softplus(dt_pre + dtb_ref[...])
    decay = jnp.exp(-jnp.exp(alog_ref[...]) * step)
    skip = jnp.broadcast_to(skip_ref[...], (bd, hd))
    by_head = jnp.concatenate([step, decay, skip], axis=0)
    by_chan = sum(jnp.dot(part, expand, preferred_element_type=F32) for part in split3(by_head))
    step_c = by_chan[0:bd]
    decay_c = by_chan[bd : 2 * bd]
    skip_c = by_chan[2 * bd : 3 * bd]
    rows = jnp.concatenate([step_c * x_conv, decay_c], axis=0)
    cols_v[...] = jnp.transpose(rows)
    xc_v[...] = skip_c * x_conv
    c_high, c_low, _ = split3(c_group)
    c_both = jnp.concatenate([c_high.astype(F32), c_low.astype(F32)], axis=0).astype(BF16)

    rows_at = 256 if di % 256 == 0 else di
    for b in range(bd):
        ready(("s", b))
        b_row = b_group[b : b + 1, :]

        def update(i, carry, b=b, b_row=b_row):
            at = pl.ds(pl.multiple_of(i * rows_at, rows_at), rows_at)
            xcol = cols_v[at, b : b + 1]
            dcol = cols_v[at, bd + b : bd + b + 1]
            new = dcol * st_ref[b, at, :] + xcol * b_row
            st_ref[b, at, :] = new
            got = lax.dot_general(
                c_both, new.astype(BF16), (((1,), (1,)), ((), ())), preferred_element_type=F32
            )
            read_v[b : b + 1, at] = got[b : b + 1, :] + got[bd + b : bd + b + 1, :]
            return carry

        lax.fori_loop(0, di // rows_at, update, 0)

    for copy in z_copies:
        copy.wait_recv()
    zall = zsend[e]
    for o in range(n_emb - 1):
        zall = zall + zrecv[o]
    gated = (read_v[...] + xc_v[...]) * silu(zall)
    total = jnp.sum(gated * gated, axis=1, keepdims=True)
    q_copies = []
    if span > 1:
        sq_send[...] = jnp.broadcast_to(total, (bd, LANES))
        for o in range(1, span):
            copy = pltpu.make_async_remote_copy(
                src_ref=sq_send,
                dst_ref=sq_recv.at[o - 1],
                send_sem=q_ss.at[o - 1],
                recv_sem=q_rs.at[o - 1],
                device_id={"heads": group * span + lax.rem(h % span + o, span)},
                device_id_type=MESH,
            )
            copy.start()
            q_copies.append(copy)
        for o, copy in enumerate(q_copies):
            copy.wait_recv()
            total = total + sq_recv[o][:, 0:1]
    inv_rms = lax.rsqrt(total / (H * P_SIZE // G) + 1e-05)
    normed = (gated * inv_rms * gain_ref[...]).astype(BF16)
    ag_v[e] = normed
    a_copies = []
    for o in range(n_emb - 1, 0, -1):
        copy = pltpu.make_async_remote_copy(
            src_ref=ag_v.at[e],
            dst_ref=ag_v.at[e],
            send_sem=a_ss.at[o - 1],
            recv_sem=a_rs.at[o - 1],
            device_id={"emb": emb_peer(o)},
            device_id_type=MESH,
        )
        copy.start()
        a_copies.append(copy)
    for copy in a_copies:
        copy.wait_recv()
    whole = jnp.concatenate([ag_v[i].astype(F32) for i in range(n_emb)], axis=0).astype(BF16)

    last = []
    own = None
    for i in range(n_out):
        ready(("o", i))
        part = jnp.dot(whole, wout_v[i], preferred_element_type=F32)
        if not fused:
            out_ref[:, i * ochunk : (i + 1) * ochunk] = part
        elif i < n_out - 1:
            rs_send[i] = part.astype(BF16)
            copy = pltpu.make_async_remote_copy(
                src_ref=rs_send.at[i],
                dst_ref=rs_recv.at[i],
                send_sem=r_ss.at[i],
                recv_sem=r_rs.at[i],
                device_id={"heads": head_peer(i + 1)},
                device_id_type=MESH,
            )
            copy.start()
            last.append(copy)
        else:
            own = part
    f_copies = []
    if fused:
        for i, copy in enumerate(last):
            copy.wait_recv()
            own = own + rs_recv[i].astype(F32)
        fin_send[...] = own.astype(BF16)
        for o in range(1, n_heads):
            copy = pltpu.make_async_remote_copy(
                src_ref=fin_send,
                dst_ref=fin_v.at[h],
                send_sem=f_ss.at[o - 1],
                recv_sem=f_rs.at[o - 1],
                device_id={"heads": head_peer(o)},
                device_id_type=MESH,
            )
            copy.start()
            f_copies.append(copy)
        fin_v[h] = fin_send[...]
        for copy in f_copies:
            copy.wait_recv()
        for i in range(n_heads):
            out_ref[:, i * ochunk : (i + 1) * ochunk] = fin_v[i]
    for copy in x_copies + z_copies + q_copies + a_copies + last + f_copies:
        copy.wait_send()


def in_hbm(*arrays):
    return [pltpu.with_memory_space_constraint(array, pltpu.HBM) for array in arrays]


def on_device(
    hidden_in,
    w_z,
    w_x,
    w_bc,
    w_dt,
    dt_bias,
    a_log,
    skip_gain,
    conv_x,
    conv_bc,
    conv_wx,
    conv_wbc,
    ssm_state,
    norm_gain,
    w_out,
):
    n_emb = lax.axis_size("emb")
    n_heads = lax.axis_size("heads")
    span = n_heads // G
    batch, depth = hidden_in.shape
    bd = conv_x.shape[0]
    k_prev = conv_x.shape[1]
    di = w_x.shape[1]
    hd = w_dt.shape[1]
    cols = w_out.shape[1]
    fused = cols % (n_heads * LANES) == 0
    chunk = min(512, di)
    ochunk = cols // n_heads if fused else min(256, cols)
    dims = (n_emb, n_heads, batch, bd, di, hd, cols, chunk, ochunk, fused, span)
    n_chunk = di // chunk
    n_out = cols // ochunk
    x_cols = di + 2 * N + LANES
    n_streams = 14 + 2 * n_chunk + bd + n_out
    vm = pl.BlockSpec(memory_space=pltpu.VMEM)
    hbm = pl.BlockSpec(memory_space=pltpu.HBM)
    dma = pltpu.SemaphoreType.DMA
    rs_n = max(n_heads - 1, 1) if fused else 1
    rs_shape = (batch, ochunk) if fused else (batch, LANES)
    fin_n = n_heads if fused else 1
    e_n = max(n_emb - 1, 1)
    q_n = max(span - 1, 1)
    out, new_state = pl.pallas_call(
        functools.partial(kernel, dims),
        out_shape=(
            jax.ShapeDtypeStruct((batch, cols), BF16 if fused else F32),
            pltpu.VMEM((bd, di, N), F32),
        ),
        in_specs=[hbm] * 15,
        out_specs=(vm, vm),
        scratch_shapes=[
            pltpu.VMEM((batch, depth), BF16),
            pltpu.VMEM((1, hd), F32),
            pltpu.VMEM((1, hd), F32),
            pltpu.VMEM((1, hd), F32),
            pltpu.VMEM((k_prev, bd, di), BF16),
            pltpu.VMEM((k_prev + 1, di), F32),
            pltpu.VMEM((1, di), F32),
            pltpu.VMEM((n_chunk, depth, chunk), BF16),
            pltpu.VMEM((n_chunk, depth, chunk), BF16),
            pltpu.VMEM((2, depth, N), BF16),
            pltpu.VMEM((hd, depth), BF16),
            pltpu.VMEM((2, k_prev, bd, N), BF16),
            pltpu.VMEM((2, k_prev + 1, N), F32),
            pltpu.VMEM((n_out, w_out.shape[0], ochunk), BF16),
            pltpu.VMEM((n_emb, bd, x_cols), F32),
            pltpu.VMEM((e_n, bd, x_cols), F32),
            pltpu.VMEM((n_emb, bd, di), F32),
            pltpu.VMEM((e_n, bd, di), F32),
            pltpu.VMEM((di, 2 * bd), F32),
            pltpu.VMEM((bd, di), F32),
            pltpu.VMEM((bd, di), F32),
            pltpu.VMEM((n_emb, bd, di), BF16),
            pltpu.VMEM((rs_n,) + rs_shape, BF16),
            pltpu.VMEM((rs_n,) + rs_shape, BF16),
            pltpu.VMEM(rs_shape, BF16),
            pltpu.VMEM((fin_n,) + rs_shape, BF16),
            pltpu.VMEM((bd, LANES), F32),
            pltpu.VMEM((q_n, bd, LANES), F32),
            dma((n_streams,)),
            dma((e_n,)),
            dma((e_n,)),
            dma((e_n,)),
            dma((e_n,)),
            dma((e_n,)),
            dma((e_n,)),
            dma((rs_n,)),
            dma((rs_n,)),
            dma((rs_n,)),
            dma((rs_n,)),
            dma((q_n,)),
            dma((q_n,)),
        ],
        compiler_params=pltpu.CompilerParams(
            collective_id=0, has_side_effects=True, vmem_limit_bytes=44 * 1024 * 1024
        ),
    )(
        *in_hbm(
        hidden_in,
        dt_bias.reshape(1, hd),
        a_log.reshape(1, hd),
        skip_gain.reshape(1, hd),
        jnp.transpose(conv_x, (1, 0, 2)),
        conv_wx,
        norm_gain.reshape(1, di),
        w_z,
        w_x,
        w_bc,
        w_dt.T,
        jnp.transpose(conv_bc, (1, 0, 2)),
        conv_wbc,
        ssm_state.reshape(bd, di, N),
        w_out,
        )
    )
    mixed = out if fused else lax.psum(out, "heads").astype(BF16)
    return (mixed, new_state.reshape(bd, hd, P_SIZE, N))


def solution(mesh):
    in_specs = (
        P(None, "emb"),
        P("emb", "heads"),
        P("emb", "heads"),
        P("emb", None),
        P("emb", "heads"),
        P("heads"),
        P("heads"),
        P("heads"),
        P("emb", None, "heads"),
        P("emb", None, None),
        P(None, "heads"),
        P(),
        P("emb", "heads", None, None),
        P("heads"),
        P("heads", "emb"),
    )
    out_specs = (P(None, "emb"), P("emb", "heads", None, None))
    return jax.shard_map(
        on_device, mesh=mesh, in_specs=in_specs, out_specs=out_specs, check_vma=False
    )
```

```python
import functools

import jax
import jax.numpy as jnp
from jax import lax
from jax.experimental import pallas as pl
from jax.experimental.pallas import tpu as pltpu
from jax.sharding import PartitionSpec as P

H = 256
P_SIZE = 64
N = 256
G = 8
LANES = 128
DEPTH = 6
MESH = pl.DeviceIdType.MESH
F32 = jnp.float32
BF16 = jnp.bfloat16


def silu(v):
    return v / (1.0 + jnp.exp(-v))


def softplus(v):
    return jnp.maximum(v, 0.0) + jnp.log1p(jnp.exp(-jnp.abs(v)))


def split3(v):
    high = v.astype(BF16)
    rest = v - high.astype(F32)
    mid = rest.astype(BF16)
    low = (rest - mid.astype(F32)).astype(BF16)
    return high, mid, low


def kernel(
    dims,
    hidden_hbm,
    dtb_hbm,
    alog_hbm,
    skip_hbm,
    convx_hbm,
    convwx_hbm,
    gain_hbm,
    wz_hbm,
    wx_hbm,
    wbc_hbm,
    wdt_hbm,
    convbc_hbm,
    convwbc_hbm,
    state_hbm,
    wout_hbm,
    out_ref,
    st_ref,
    hidden_ref,
    dtb_ref,
    alog_ref,
    skip_ref,
    convx_v,
    convwx_ref,
    gain_ref,
    wz_v,
    wx_v,
    wbc_v,
    wdt_v,
    convbc_v,
    convwbc_v,
    wout_v,
    xsend,
    xrecv,
    zsend,
    zrecv,
    cols_v,
    read_v,
    xc_v,
    ag_v,
    rs_send,
    rs_recv,
    fin_send,
    fin_v,
    sq_send,
    sq_recv,
    dma_sem,
    x_ss,
    x_rs,
    z_ss,
    z_rs,
    a_ss,
    a_rs,
    r_ss,
    r_rs,
    f_ss,
    f_rs,
    q_ss,
    q_rs,
):
    n_emb, n_heads, batch, bd, di, hd, cols, chunk, ochunk, fused, span = dims
    e = lax.axis_index("emb")
    h = lax.axis_index("heads")
    group = h // span

    def emb_peer(o):
        return lax.rem(e + o, n_emb)

    def head_peer(mask):
        peer = h
        bit = 1
        while bit < n_heads:
            if mask & bit:
                peer = peer + bit * (1 - 2 * lax.rem(lax.div(h, bit), 2))
            bit *= 2
        return peer

    copies = {}
    order = []

    def stream(name, src, dst):
        copies[name] = pltpu.make_async_copy(src, dst, dma_sem.at[len(order)])
        order.append(name)

    stream("hidden", hidden_hbm, hidden_ref)
    for half in range(2):
        off = pl.multiple_of(half * G * N + group * N, N)
        stream(("bc", half), wbc_hbm.at[:, pl.ds(off, N)], wbc_v.at[half])
    stream(("dt", 0), wdt_hbm, wdt_v)
    for half in range(2):
        off = pl.multiple_of(half * G * N + group * N, N)
        stream(("cb", half), convbc_hbm.at[:, :, pl.ds(off, N)], convbc_v.at[half])
        stream(("cw", half), convwbc_hbm.at[:, pl.ds(off, N)], convwbc_v.at[half])
    stream("dtb", dtb_hbm, dtb_ref)
    stream("alog", alog_hbm, alog_ref)
    stream("skip", skip_hbm, skip_ref)
    stream("convx", convx_hbm, convx_v)
    stream("convwx", convwx_hbm, convwx_ref)
    stream("gain", gain_hbm, gain_ref)
    n_chunk = di // chunk
    for c in range(n_chunk):
        stream(("x", c), wx_hbm.at[:, pl.ds(c * chunk, chunk)], wx_v.at[c])
    for c in range(n_chunk):
        stream(("z", c), wz_hbm.at[:, pl.ds(c * chunk, chunk)], wz_v.at[c])
    rows_in = min(512, di)
    for i in range(di // rows_in):
        part = pl.ds(i * rows_in, rows_in)
        stream(("s", i), state_hbm.at[:, part], st_ref.at[:, part])
    n_out = cols // ochunk
    for i in range(n_out):
        at = head_peer(n_heads - 1 - i) if fused else i
        off = pl.multiple_of(at * ochunk, ochunk)
        stream(("o", i), wout_hbm.at[:, pl.ds(off, ochunk)], wout_v.at[i])
    started = [0]

    def advance():
        if started[0] < len(order):
            copies[order[started[0]]].start()
            started[0] += 1

    def ready(name):
        copies[name].wait()
        advance()

    for _ in range(DEPTH + 12):
        advance()

    barrier = pltpu.get_barrier_semaphore()
    for o in range(1, n_emb):
        pl.semaphore_signal(barrier, inc=1, device_id={"emb": emb_peer(o)}, device_id_type=MESH)
    n_greet = n_emb - 1
    if fused:
        for o in range(1, n_heads):
            pl.semaphore_signal(
                barrier, inc=1, device_id={"heads": head_peer(o)}, device_id_type=MESH
            )
        n_greet += n_heads - 1
    elif span > 1:
        for o in range(1, span):
            pl.semaphore_signal(
                barrier,
                inc=1,
                device_id={"heads": group * span + lax.rem(h % span + o, span)},
                device_id_type=MESH,
            )
        n_greet += span - 1

    ready("hidden")
    hidden = hidden_ref[...]

    def project(weights, send, at, width):
        part = jnp.dot(hidden, weights, preferred_element_type=F32)
        for peer in range(n_emb):
            send[peer, :, at : at + width] = part[peer * bd : (peer + 1) * bd]

    heads_at = lax.broadcasted_iota(jnp.int32, (hd, di), 0)
    chans_at = lax.broadcasted_iota(jnp.int32, (hd, di), 1)
    lower = heads_at * P_SIZE
    expand = jnp.where((chans_at >= lower) & (chans_at < lower + P_SIZE), 1.0, 0.0).astype(BF16)

    k_prev = convx_v.shape[0]

    def conv_prev(values, taps):
        return sum(values[k].astype(F32) * taps[k : k + 1, :] for k in range(k_prev))

    for half in range(2):
        ready(("bc", half))
        project(wbc_v[half], xsend, di + half * N, N)
    ready(("dt", 0))
    xsend[:, :, di + 2 * N :] = jnp.zeros((n_emb, bd, LANES), F32)
    part = lax.dot_general(
        hidden, wdt_v[...], (((1,), (1,)), ((), ())), preferred_element_type=F32
    )
    for peer in range(n_emb):
        xsend[peer, :, di + 2 * N : di + 2 * N + hd] = part[peer * bd : (peer + 1) * bd]
    bc_base = []
    for half in range(2):
        ready(("cb", half))
        ready(("cw", half))
        bc_base.append(conv_prev(convbc_v.at[half], convwbc_v[half]))
    for name in ("dtb", "alog", "skip", "convx", "convwx", "gain"):
        ready(name)
    x_base = conv_prev(convx_v, convwx_ref[...])
    for c in range(n_chunk):
        ready(("x", c))
        project(wx_v[c], xsend, c * chunk, chunk)

    pl.semaphore_wait(barrier, n_greet)

    def send_emb(src, dst, ss, rs):
        made = []
        for o in range(n_emb - 1, 0, -1):
            peer = emb_peer(o)
            copy = pltpu.make_async_remote_copy(
                src_ref=src.at[peer],
                dst_ref=dst.at[o - 1],
                send_sem=ss.at[o - 1],
                recv_sem=rs.at[o - 1],
                device_id={"emb": peer},
                device_id_type=MESH,
            )
            copy.start()
            made.append(copy)
        return made

    x_copies = send_emb(xsend, xrecv, x_ss, x_rs)
    for c in range(n_chunk):
        ready(("z", c))
        project(wz_v[c], zsend, c * chunk, chunk)
    z_copies = send_emb(zsend, zrecv, z_ss, z_rs)

    for copy in x_copies:
        copy.wait_recv()
    xall = xsend[e]
    for o in range(n_emb - 1):
        xall = xall + xrecv[o]
    x_conv = silu(x_base + xall[:, 0:di] * convwx_ref[k_prev : k_prev + 1, :])
    bc = []
    for half in range(2):
        pre = xall[:, di + half * N : di + (half + 1) * N]
        bc.append(silu(bc_base[half] + pre * convwbc_v[half, k_prev : k_prev + 1, :]))
    b_group, c_group = bc
    dt_pre = xall[:, di + 2 * N : di + 2 * N + hd]
    step = softplus(dt_pre + dtb_ref[...])
    decay = jnp.exp(-jnp.exp(alog_ref[...]) * step)
    skip = jnp.broadcast_to(skip_ref[...], (bd, hd))
    by_head = jnp.concatenate([step, decay, skip], axis=0)
    by_chan = sum(jnp.dot(part, expand, preferred_element_type=F32) for part in split3(by_head))
    step_c = by_chan[0:bd]
    decay_c = by_chan[bd : 2 * bd]
    skip_c = by_chan[2 * bd : 3 * bd]
    rows = jnp.concatenate([step_c * x_conv, decay_c], axis=0)
    cols_v[...] = jnp.transpose(rows)
    xc_v[...] = skip_c * x_conv
    c_high, c_low, _ = split3(c_group)
    c_both = jnp.concatenate([c_high.astype(F32), c_low.astype(F32)], axis=0).astype(BF16)

    rows_at = min(256, rows_in)
    lane = lax.broadcasted_iota(jnp.int32, (rows_at, 2 * bd), 1)
    for i in range(di // rows_in):
        ready(("s", i))

        def update(j, carry, i=i):
            at = pl.ds(pl.multiple_of(i * rows_in + j * rows_at, rows_at), rows_at)
            found = None
            for b in range(bd):
                xcol = cols_v[at, b : b + 1]
                dcol = cols_v[at, bd + b : bd + b + 1]
                new = dcol * st_ref[b, at, :] + xcol * b_group[b : b + 1, :]
                st_ref[b, at, :] = new
                got = lax.dot_general(
                    new.astype(BF16), c_both, (((1,), (1,)), ((), ())), preferred_element_type=F32
                )
                mine = (lane == b) | (lane == bd + b)
                found = got if found is None else jnp.where(mine, got, found)
            read_v[at, :] = found
            return carry

        lax.fori_loop(0, rows_in // rows_at, update, 0)
    read_rows = jnp.transpose(read_v[...])
    read = read_rows[0:bd] + read_rows[bd : 2 * bd]

    for copy in z_copies:
        copy.wait_recv()
    zall = zsend[e]
    for o in range(n_emb - 1):
        zall = zall + zrecv[o]
    gated = (read + xc_v[...]) * silu(zall)
    total = jnp.sum(gated * gated, axis=1, keepdims=True)
    q_copies = []
    if span > 1:
        sq_send[...] = jnp.broadcast_to(total, (bd, LANES))
        for o in range(1, span):
            copy = pltpu.make_async_remote_copy(
                src_ref=sq_send,
                dst_ref=sq_recv.at[o - 1],
                send_sem=q_ss.at[o - 1],
                recv_sem=q_rs.at[o - 1],
                device_id={"heads": group * span + lax.rem(h % span + o, span)},
                device_id_type=MESH,
            )
            copy.start()
            q_copies.append(copy)
        for o, copy in enumerate(q_copies):
            copy.wait_recv()
            total = total + sq_recv[o][:, 0:1]
    inv_rms = lax.rsqrt(total / (H * P_SIZE // G) + 1e-05)
    normed = (gated * inv_rms * gain_ref[...]).astype(BF16)
    ag_v[e] = normed
    a_copies = []
    for o in range(n_emb - 1, 0, -1):
        copy = pltpu.make_async_remote_copy(
            src_ref=ag_v.at[e],
            dst_ref=ag_v.at[e],
            send_sem=a_ss.at[o - 1],
            recv_sem=a_rs.at[o - 1],
            device_id={"emb": emb_peer(o)},
            device_id_type=MESH,
        )
        copy.start()
        a_copies.append(copy)
    for copy in a_copies:
        copy.wait_recv()
    whole = jnp.concatenate([ag_v[i].astype(F32) for i in range(n_emb)], axis=0).astype(BF16)

    last = []
    own = None
    for i in range(n_out):
        ready(("o", i))
        part = jnp.dot(whole, wout_v[i], preferred_element_type=F32)
        if not fused:
            out_ref[:, i * ochunk : (i + 1) * ochunk] = part
        elif i < n_out - 1:
            rs_send[i] = part.astype(BF16)
            copy = pltpu.make_async_remote_copy(
                src_ref=rs_send.at[i],
                dst_ref=rs_recv.at[i],
                send_sem=r_ss.at[i],
                recv_sem=r_rs.at[i],
                device_id={"heads": head_peer(n_heads - 1 - i)},
                device_id_type=MESH,
            )
            copy.start()
            last.append(copy)
        else:
            own = part
    f_copies = []
    if fused:
        for i, copy in enumerate(last):
            copy.wait_recv()
            own = own + rs_recv[i].astype(F32)
        fin_send[...] = own.astype(BF16)
        for o in range(n_heads - 1, 0, -1):
            copy = pltpu.make_async_remote_copy(
                src_ref=fin_send,
                dst_ref=fin_v.at[h],
                send_sem=f_ss.at[o - 1],
                recv_sem=f_rs.at[o - 1],
                device_id={"heads": head_peer(o)},
                device_id_type=MESH,
            )
            copy.start()
            f_copies.append(copy)
        fin_v[h] = fin_send[...]
        for copy in f_copies:
            copy.wait_recv()
        for i in range(n_heads):
            out_ref[:, i * ochunk : (i + 1) * ochunk] = fin_v[i]
    for copy in x_copies + z_copies + q_copies + a_copies + last + f_copies:
        copy.wait_send()


def in_hbm(*arrays):
    return [pltpu.with_memory_space_constraint(array, pltpu.HBM) for array in arrays]


def on_device(
    hidden_in,
    w_z,
    w_x,
    w_bc,
    w_dt,
    dt_bias,
    a_log,
    skip_gain,
    conv_x,
    conv_bc,
    conv_wx,
    conv_wbc,
    ssm_state,
    norm_gain,
    w_out,
):
    n_emb = lax.axis_size("emb")
    n_heads = lax.axis_size("heads")
    span = n_heads // G
    batch, depth = hidden_in.shape
    bd = conv_x.shape[0]
    k_prev = conv_x.shape[1]
    di = w_x.shape[1]
    hd = w_dt.shape[1]
    cols = w_out.shape[1]
    fused = cols % (n_heads * LANES) == 0
    chunk = min(512, di)
    ochunk = cols // n_heads if fused else min(256, cols)
    dims = (n_emb, n_heads, batch, bd, di, hd, cols, chunk, ochunk, fused, span)
    n_chunk = di // chunk
    n_out = cols // ochunk
    x_cols = di + 2 * N + LANES
    n_streams = 14 + 2 * n_chunk + di // min(512, di) + n_out
    vm = pl.BlockSpec(memory_space=pltpu.VMEM)
    hbm = pl.BlockSpec(memory_space=pltpu.HBM)
    dma = pltpu.SemaphoreType.DMA
    rs_n = max(n_heads - 1, 1) if fused else 1
    rs_shape = (batch, ochunk) if fused else (batch, LANES)
    fin_n = n_heads if fused else 1
    e_n = max(n_emb - 1, 1)
    q_n = max(span - 1, 1)
    out, new_state = pl.pallas_call(
        functools.partial(kernel, dims),
        out_shape=(
            jax.ShapeDtypeStruct((batch, cols), BF16 if fused else F32),
            pltpu.VMEM((bd, di, N), F32),
        ),
        in_specs=[hbm] * 15,
        out_specs=(vm, vm),
        scratch_shapes=[
            pltpu.VMEM((batch, depth), BF16),
            pltpu.VMEM((1, hd), F32),
            pltpu.VMEM((1, hd), F32),
            pltpu.VMEM((1, hd), F32),
            pltpu.VMEM((k_prev, bd, di), BF16),
            pltpu.VMEM((k_prev + 1, di), F32),
            pltpu.VMEM((1, di), F32),
            pltpu.VMEM((n_chunk, depth, chunk), BF16),
            pltpu.VMEM((n_chunk, depth, chunk), BF16),
            pltpu.VMEM((2, depth, N), BF16),
            pltpu.VMEM((hd, depth), BF16),
            pltpu.VMEM((2, k_prev, bd, N), BF16),
            pltpu.VMEM((2, k_prev + 1, N), F32),
            pltpu.VMEM((n_out, w_out.shape[0], ochunk), BF16),
            pltpu.VMEM((n_emb, bd, x_cols), F32),
            pltpu.VMEM((e_n, bd, x_cols), F32),
            pltpu.VMEM((n_emb, bd, di), F32),
            pltpu.VMEM((e_n, bd, di), F32),
            pltpu.VMEM((di, 2 * bd), F32),
            pltpu.VMEM((di, 2 * bd), F32),
            pltpu.VMEM((bd, di), F32),
            pltpu.VMEM((n_emb, bd, di), BF16),
            pltpu.VMEM((rs_n,) + rs_shape, BF16),
            pltpu.VMEM((rs_n,) + rs_shape, BF16),
            pltpu.VMEM(rs_shape, BF16),
            pltpu.VMEM((fin_n,) + rs_shape, BF16),
            pltpu.VMEM((bd, LANES), F32),
            pltpu.VMEM((q_n, bd, LANES), F32),
            dma((n_streams,)),
            dma((e_n,)),
            dma((e_n,)),
            dma((e_n,)),
            dma((e_n,)),
            dma((e_n,)),
            dma((e_n,)),
            dma((rs_n,)),
            dma((rs_n,)),
            dma((rs_n,)),
            dma((rs_n,)),
            dma((q_n,)),
            dma((q_n,)),
        ],
        compiler_params=pltpu.CompilerParams(
            collective_id=0, has_side_effects=True, vmem_limit_bytes=44 * 1024 * 1024
        ),
    )(
        *in_hbm(
        hidden_in,
        dt_bias.reshape(1, hd),
        a_log.reshape(1, hd),
        skip_gain.reshape(1, hd),
        jnp.transpose(conv_x, (1, 0, 2)),
        conv_wx,
        norm_gain.reshape(1, di),
        w_z,
        w_x,
        w_bc,
        w_dt.T,
        jnp.transpose(conv_bc, (1, 0, 2)),
        conv_wbc,
        ssm_state.reshape(bd, di, N),
        w_out,
        )
    )
    mixed = out if fused else lax.psum(out, "heads").astype(BF16)
    return (mixed, new_state.reshape(bd, hd, P_SIZE, N))


def solution(mesh):
    in_specs = (
        P(None, "emb"),
        P("emb", "heads"),
        P("emb", "heads"),
        P("emb", None),
        P("emb", "heads"),
        P("heads"),
        P("heads"),
        P("heads"),
        P("emb", None, "heads"),
        P("emb", None, None),
        P(None, "heads"),
        P(),
        P("emb", "heads", None, None),
        P("heads"),
        P("heads", "emb"),
    )
    out_specs = (P(None, "emb"), P("emb", "heads", None, None))
    return jax.shard_map(
        on_device, mesh=mesh, in_specs=in_specs, out_specs=out_specs, check_vma=False
    )
```

```python
import functools

import jax
import jax.numpy as jnp
from jax import lax
from jax.experimental import pallas as pl
from jax.experimental.pallas import tpu as pltpu
from jax.sharding import PartitionSpec as P

H = 256
P_SIZE = 64
N = 256
G = 8
LANES = 128
DEPTH = 6
MESH = pl.DeviceIdType.MESH
F32 = jnp.float32
BF16 = jnp.bfloat16


def silu(v):
    return v / (1.0 + jnp.exp(-v))


def softplus(v):
    return jnp.maximum(v, 0.0) + jnp.log1p(jnp.exp(-jnp.abs(v)))


def split3(v):
    high = v.astype(BF16)
    rest = v - high.astype(F32)
    mid = rest.astype(BF16)
    low = (rest - mid.astype(F32)).astype(BF16)
    return high, mid, low


def kernel(
    dims,
    hidden_hbm,
    dtb_hbm,
    alog_hbm,
    skip_hbm,
    convx_hbm,
    convwx_hbm,
    gain_hbm,
    wz_hbm,
    wx_hbm,
    wbc_hbm,
    wdt_hbm,
    convbc_hbm,
    convwbc_hbm,
    state_hbm,
    wout_hbm,
    out_ref,
    st_ref,
    hidden_ref,
    dtb_ref,
    alog_ref,
    skip_ref,
    convx_v,
    convwx_ref,
    gain_ref,
    wz_v,
    wx_v,
    wbc_v,
    wdt_v,
    convbc_v,
    convwbc_v,
    wout_v,
    xsend,
    xrecv,
    zsend,
    zrecv,
    cols_v,
    read_v,
    xc_v,
    ag_v,
    rs_send,
    rs_recv,
    fin_send,
    fin_v,
    sq_send,
    sq_recv,
    dma_sem,
    x_ss,
    x_rs,
    z_ss,
    z_rs,
    a_ss,
    a_rs,
    r_ss,
    r_rs,
    f_ss,
    f_rs,
    q_ss,
    q_rs,
):
    n_emb, n_heads, batch, bd, di, hd, cols, chunk, ochunk, fused, span = dims
    e = lax.axis_index("emb")
    h = lax.axis_index("heads")
    group = h // span

    def emb_peer(o):
        return lax.rem(e + o, n_emb)

    def head_peer(mask):
        peer = h
        bit = 1
        while bit < n_heads:
            if mask & bit:
                peer = peer + bit * (1 - 2 * lax.rem(lax.div(h, bit), 2))
            bit *= 2
        return peer

    copies = {}
    order = []

    def stream(name, src, dst):
        copies[name] = pltpu.make_async_copy(src, dst, dma_sem.at[len(order)])
        order.append(name)

    stream("hidden", hidden_hbm, hidden_ref)
    for half in range(2):
        off = pl.multiple_of(half * G * N + group * N, N)
        stream(("bc", half), wbc_hbm.at[:, pl.ds(off, N)], wbc_v.at[half])
    stream(("dt", 0), wdt_hbm, wdt_v)
    for half in range(2):
        off = pl.multiple_of(half * G * N + group * N, N)
        stream(("cb", half), convbc_hbm.at[:, :, pl.ds(off, N)], convbc_v.at[half])
        stream(("cw", half), convwbc_hbm.at[:, pl.ds(off, N)], convwbc_v.at[half])
    stream("dtb", dtb_hbm, dtb_ref)
    stream("alog", alog_hbm, alog_ref)
    stream("skip", skip_hbm, skip_ref)
    stream("convx", convx_hbm, convx_v)
    stream("convwx", convwx_hbm, convwx_ref)
    stream("gain", gain_hbm, gain_ref)
    n_chunk = di // chunk
    for c in range(n_chunk):
        stream(("x", c), wx_hbm.at[:, pl.ds(c * chunk, chunk)], wx_v.at[c])
    for c in range(n_chunk):
        stream(("z", c), wz_hbm.at[:, pl.ds(c * chunk, chunk)], wz_v.at[c])
    rows_in = min(512, di)
    for i in range(di // rows_in):
        part = pl.ds(i * rows_in, rows_in)
        stream(("s", i), state_hbm.at[:, part], st_ref.at[:, part])
    n_out = cols // ochunk
    for i in range(n_out):
        at = head_peer(n_heads - 1 - i) if fused else i
        off = pl.multiple_of(at * ochunk, ochunk)
        stream(("o", i), wout_hbm.at[:, pl.ds(off, ochunk)], wout_v.at[i])
    started = [0]

    def advance():
        if started[0] < len(order):
            copies[order[started[0]]].start()
            started[0] += 1

    def ready(name):
        copies[name].wait()
        if name[0] in ("bc", "x", "z", "s", "o"):
            advance()

    for _ in range(DEPTH + 12):
        advance()

    barrier = pltpu.get_barrier_semaphore()
    for o in range(1, n_emb):
        pl.semaphore_signal(barrier, inc=1, device_id={"emb": emb_peer(o)}, device_id_type=MESH)
    n_greet = n_emb - 1
    if fused:
        for o in range(1, n_heads):
            pl.semaphore_signal(
                barrier, inc=1, device_id={"heads": head_peer(o)}, device_id_type=MESH
            )
        n_greet += n_heads - 1
    elif span > 1:
        for o in range(1, span):
            pl.semaphore_signal(
                barrier,
                inc=1,
                device_id={"heads": group * span + lax.rem(h % span + o, span)},
                device_id_type=MESH,
            )
        n_greet += span - 1

    ready("hidden")
    hidden = hidden_ref[...]

    def project(weights, send, at, width):
        part = jnp.dot(hidden, weights, preferred_element_type=F32)
        for peer in range(n_emb):
            send[peer, :, at : at + width] = part[peer * bd : (peer + 1) * bd]

    heads_at = lax.broadcasted_iota(jnp.int32, (hd, di), 0)
    chans_at = lax.broadcasted_iota(jnp.int32, (hd, di), 1)
    lower = heads_at * P_SIZE
    expand = jnp.where((chans_at >= lower) & (chans_at < lower + P_SIZE), 1.0, 0.0).astype(BF16)

    k_prev = convx_v.shape[0]

    def conv_prev(values, taps):
        return sum(values[k].astype(F32) * taps[k : k + 1, :] for k in range(k_prev))

    for half in range(2):
        ready(("bc", half))
        project(wbc_v[half], xsend, di + half * N, N)
    ready(("dt", 0))
    xsend[:, :, di + 2 * N :] = jnp.zeros((n_emb, bd, LANES), F32)
    part = lax.dot_general(
        hidden, wdt_v[...], (((1,), (1,)), ((), ())), preferred_element_type=F32
    )
    for peer in range(n_emb):
        xsend[peer, :, di + 2 * N : di + 2 * N + hd] = part[peer * bd : (peer + 1) * bd]
    bc_base = []
    for half in range(2):
        ready(("cb", half))
        ready(("cw", half))
        bc_base.append(conv_prev(convbc_v.at[half], convwbc_v[half]))
    for name in ("dtb", "alog", "skip", "convx", "convwx", "gain"):
        ready(name)
    x_base = conv_prev(convx_v, convwx_ref[...])
    for c in range(n_chunk):
        ready(("x", c))
        project(wx_v[c], xsend, c * chunk, chunk)

    pl.semaphore_wait(barrier, n_greet)

    def send_emb(src, dst, ss, rs):
        made = []
        for o in range(n_emb - 1, 0, -1):
            peer = emb_peer(o)
            copy = pltpu.make_async_remote_copy(
                src_ref=src.at[peer],
                dst_ref=dst.at[o - 1],
                send_sem=ss.at[o - 1],
                recv_sem=rs.at[o - 1],
                device_id={"emb": peer},
                device_id_type=MESH,
            )
            copy.start()
            made.append(copy)
        return made

    x_copies = send_emb(xsend, xrecv, x_ss, x_rs)
    for c in range(n_chunk):
        ready(("z", c))
        project(wz_v[c], zsend, c * chunk, chunk)
    z_copies = send_emb(zsend, zrecv, z_ss, z_rs)

    for copy in x_copies:
        copy.wait_recv()
    xall = xsend[e]
    for o in range(n_emb - 1):
        xall = xall + xrecv[o]
    x_conv = silu(x_base + xall[:, 0:di] * convwx_ref[k_prev : k_prev + 1, :])
    bc = []
    for half in range(2):
        pre = xall[:, di + half * N : di + (half + 1) * N]
        bc.append(silu(bc_base[half] + pre * convwbc_v[half, k_prev : k_prev + 1, :]))
    b_group, c_group = bc
    dt_pre = xall[:, di + 2 * N : di + 2 * N + hd]
    step = softplus(dt_pre + dtb_ref[...])
    decay = jnp.exp(-jnp.exp(alog_ref[...]) * step)
    skip = jnp.broadcast_to(skip_ref[...], (bd, hd))
    by_head = jnp.concatenate([step, decay, skip], axis=0)
    by_chan = sum(jnp.dot(part, expand, preferred_element_type=F32) for part in split3(by_head))
    step_c = by_chan[0:bd]
    decay_c = by_chan[bd : 2 * bd]
    skip_c = by_chan[2 * bd : 3 * bd]
    rows = jnp.concatenate([step_c * x_conv, decay_c], axis=0)
    cols_v[...] = jnp.transpose(rows)
    xc_v[...] = skip_c * x_conv
    c_high, c_low, _ = split3(c_group)
    c_both = jnp.concatenate([c_high.astype(F32), c_low.astype(F32)], axis=0).astype(BF16)

    rows_at = min(256, rows_in)
    lane = lax.broadcasted_iota(jnp.int32, (rows_at, 2 * bd), 1)
    for i in range(di // rows_in):
        ready(("s", i))

        def update(j, carry, i=i):
            at = pl.ds(pl.multiple_of(i * rows_in + j * rows_at, rows_at), rows_at)
            found = None
            for b in range(bd):
                xcol = cols_v[at, b : b + 1]
                dcol = cols_v[at, bd + b : bd + b + 1]
                new = dcol * st_ref[b, at, :] + xcol * b_group[b : b + 1, :]
                st_ref[b, at, :] = new
                got = lax.dot_general(
                    new.astype(BF16), c_both, (((1,), (1,)), ((), ())), preferred_element_type=F32
                )
                mine = (lane == b) | (lane == bd + b)
                found = got if found is None else jnp.where(mine, got, found)
            read_v[at, :] = found
            return carry

        lax.fori_loop(0, rows_in // rows_at, update, 0)
    read_rows = jnp.transpose(read_v[...])
    read = read_rows[0:bd] + read_rows[bd : 2 * bd]

    for copy in z_copies:
        copy.wait_recv()
    zall = zsend[e]
    for o in range(n_emb - 1):
        zall = zall + zrecv[o]
    gated = (read + xc_v[...]) * silu(zall)
    total = jnp.sum(gated * gated, axis=1, keepdims=True)
    q_copies = []
    if span > 1:
        sq_send[...] = jnp.broadcast_to(total, (bd, LANES))
        for o in range(1, span):
            copy = pltpu.make_async_remote_copy(
                src_ref=sq_send,
                dst_ref=sq_recv.at[o - 1],
                send_sem=q_ss.at[o - 1],
                recv_sem=q_rs.at[o - 1],
                device_id={"heads": group * span + lax.rem(h % span + o, span)},
                device_id_type=MESH,
            )
            copy.start()
            q_copies.append(copy)
        for o, copy in enumerate(q_copies):
            copy.wait_recv()
            total = total + sq_recv[o][:, 0:1]
    inv_rms = lax.rsqrt(total / (H * P_SIZE // G) + 1e-05)
    normed = (gated * inv_rms * gain_ref[...]).astype(BF16)
    ag_v[e] = normed
    a_copies = []
    for o in range(n_emb - 1, 0, -1):
        copy = pltpu.make_async_remote_copy(
            src_ref=ag_v.at[e],
            dst_ref=ag_v.at[e],
            send_sem=a_ss.at[o - 1],
            recv_sem=a_rs.at[o - 1],
            device_id={"emb": emb_peer(o)},
            device_id_type=MESH,
        )
        copy.start()
        a_copies.append(copy)
    for copy in a_copies:
        copy.wait_recv()
    whole = jnp.concatenate([ag_v[i].astype(F32) for i in range(n_emb)], axis=0).astype(BF16)

    last = []
    own = None
    for i in range(n_out):
        ready(("o", i))
        part = jnp.dot(whole, wout_v[i], preferred_element_type=F32)
        if not fused:
            out_ref[:, i * ochunk : (i + 1) * ochunk] = part
        elif i < n_out - 1:
            rs_send[i] = part.astype(BF16)
            copy = pltpu.make_async_remote_copy(
                src_ref=rs_send.at[i],
                dst_ref=rs_recv.at[i],
                send_sem=r_ss.at[i],
                recv_sem=r_rs.at[i],
                device_id={"heads": head_peer(n_heads - 1 - i)},
                device_id_type=MESH,
            )
            copy.start()
            last.append(copy)
        else:
            own = part
    f_copies = []
    if fused:
        for i, copy in enumerate(last):
            copy.wait_recv()
            own = own + rs_recv[i].astype(F32)
        fin_send[...] = own.astype(BF16)
        for o in range(n_heads - 1, 0, -1):
            copy = pltpu.make_async_remote_copy(
                src_ref=fin_send,
                dst_ref=fin_v.at[h],
                send_sem=f_ss.at[o - 1],
                recv_sem=f_rs.at[o - 1],
                device_id={"heads": head_peer(o)},
                device_id_type=MESH,
            )
            copy.start()
            f_copies.append(copy)
        fin_v[h] = fin_send[...]
        for copy in f_copies:
            copy.wait_recv()
        for i in range(n_heads):
            out_ref[:, i * ochunk : (i + 1) * ochunk] = fin_v[i]
    for copy in x_copies + z_copies + q_copies + a_copies + last + f_copies:
        copy.wait_send()


def in_hbm(*arrays):
    return [pltpu.with_memory_space_constraint(array, pltpu.HBM) for array in arrays]


def on_device(
    hidden_in,
    w_z,
    w_x,
    w_bc,
    w_dt,
    dt_bias,
    a_log,
    skip_gain,
    conv_x,
    conv_bc,
    conv_wx,
    conv_wbc,
    ssm_state,
    norm_gain,
    w_out,
):
    n_emb = lax.axis_size("emb")
    n_heads = lax.axis_size("heads")
    span = n_heads // G
    batch, depth = hidden_in.shape
    bd = conv_x.shape[0]
    k_prev = conv_x.shape[1]
    di = w_x.shape[1]
    hd = w_dt.shape[1]
    cols = w_out.shape[1]
    fused = cols % (n_heads * LANES) == 0
    chunk = min(512, di)
    ochunk = cols // n_heads if fused else min(256, cols)
    dims = (n_emb, n_heads, batch, bd, di, hd, cols, chunk, ochunk, fused, span)
    n_chunk = di // chunk
    n_out = cols // ochunk
    x_cols = di + 2 * N + LANES
    n_streams = 14 + 2 * n_chunk + di // min(512, di) + n_out
    vm = pl.BlockSpec(memory_space=pltpu.VMEM)
    hbm = pl.BlockSpec(memory_space=pltpu.HBM)
    dma = pltpu.SemaphoreType.DMA
    rs_n = max(n_heads - 1, 1) if fused else 1
    rs_shape = (batch, ochunk) if fused else (batch, LANES)
    fin_n = n_heads if fused else 1
    e_n = max(n_emb - 1, 1)
    q_n = max(span - 1, 1)
    out, new_state = pl.pallas_call(
        functools.partial(kernel, dims),
        out_shape=(
            jax.ShapeDtypeStruct((batch, cols), BF16 if fused else F32),
            pltpu.VMEM((bd, di, N), F32),
        ),
        in_specs=[hbm] * 15,
        out_specs=(vm, vm),
        scratch_shapes=[
            pltpu.VMEM((batch, depth), BF16),
            pltpu.VMEM((1, hd), F32),
            pltpu.VMEM((1, hd), F32),
            pltpu.VMEM((1, hd), F32),
            pltpu.VMEM((k_prev, bd, di), BF16),
            pltpu.VMEM((k_prev + 1, di), F32),
            pltpu.VMEM((1, di), F32),
            pltpu.VMEM((n_chunk, depth, chunk), BF16),
            pltpu.VMEM((n_chunk, depth, chunk), BF16),
            pltpu.VMEM((2, depth, N), BF16),
            pltpu.VMEM((hd, depth), BF16),
            pltpu.VMEM((2, k_prev, bd, N), BF16),
            pltpu.VMEM((2, k_prev + 1, N), F32),
            pltpu.VMEM((n_out, w_out.shape[0], ochunk), BF16),
            pltpu.VMEM((n_emb, bd, x_cols), F32),
            pltpu.VMEM((e_n, bd, x_cols), F32),
            pltpu.VMEM((n_emb, bd, di), F32),
            pltpu.VMEM((e_n, bd, di), F32),
            pltpu.VMEM((di, 2 * bd), F32),
            pltpu.VMEM((di, 2 * bd), F32),
            pltpu.VMEM((bd, di), F32),
            pltpu.VMEM((n_emb, bd, di), BF16),
            pltpu.VMEM((rs_n,) + rs_shape, BF16),
            pltpu.VMEM((rs_n,) + rs_shape, BF16),
            pltpu.VMEM(rs_shape, BF16),
            pltpu.VMEM((fin_n,) + rs_shape, BF16),
            pltpu.VMEM((bd, LANES), F32),
            pltpu.VMEM((q_n, bd, LANES), F32),
            dma((n_streams,)),
            dma((e_n,)),
            dma((e_n,)),
            dma((e_n,)),
            dma((e_n,)),
            dma((e_n,)),
            dma((e_n,)),
            dma((rs_n,)),
            dma((rs_n,)),
            dma((rs_n,)),
            dma((rs_n,)),
            dma((q_n,)),
            dma((q_n,)),
        ],
        compiler_params=pltpu.CompilerParams(
            collective_id=0, has_side_effects=True, vmem_limit_bytes=44 * 1024 * 1024
        ),
    )(
        *in_hbm(
        hidden_in,
        dt_bias.reshape(1, hd),
        a_log.reshape(1, hd),
        skip_gain.reshape(1, hd),
        jnp.transpose(conv_x, (1, 0, 2)),
        conv_wx,
        norm_gain.reshape(1, di),
        w_z,
        w_x,
        w_bc,
        w_dt.T,
        jnp.transpose(conv_bc, (1, 0, 2)),
        conv_wbc,
        ssm_state.reshape(bd, di, N),
        w_out,
        )
    )
    mixed = out if fused else lax.psum(out, "heads").astype(BF16)
    return (mixed, new_state.reshape(bd, hd, P_SIZE, N))


def solution(mesh):
    in_specs = (
        P(None, "emb"),
        P("emb", "heads"),
        P("emb", "heads"),
        P("emb", None),
        P("emb", "heads"),
        P("heads"),
        P("heads"),
        P("heads"),
        P("emb", None, "heads"),
        P("emb", None, None),
        P(None, "heads"),
        P(),
        P("emb", "heads", None, None),
        P("heads"),
        P("heads", "emb"),
    )
    out_specs = (P(None, "emb"), P("emb", "heads", None, None))
    return jax.shard_map(
        on_device, mesh=mesh, in_specs=in_specs, out_specs=out_specs, check_vma=False
    )
```
